8 devices in a mesh: dp: 1 (over z), tp: 8 (over y, x, core).
Axes of the slice: x: 2, y: 2, z: 1, core: 2. Of those that a mesh axis runs over, the one named last changes fastest.
Arguments:
- y_one: float32 [16, 256, 1024], P('dp')
- y_two: float32 [16, 256, 1024], P('dp')
- dy_one: float32 [16, 256, 1024], P('dp')
- dy_two: float32 [16, 256, 1024], P('dp')
- saved_one: float32 [2, 16, 256, 1024], P(None, 'dp')
- saved_two: float32 [2, 16, 256, 1024], P(None, 'dp')
- w_qkv: bfloat16 [5, 1024, 3, 16, 64], P(None, None, None, 'tp')
- w_o: bfloat16 [5, 16, 64, 1024], P(None, 'tp')
- w_in: bfloat16 [5, 1024, 4096], P(None, None, 'tp')
- w_out: bfloat16 [5, 4096, 1024], P(None, 'tp')
Outputs:
- output 1: float32 [16, 256, 1024], P('dp')
- output 2: float32 [16, 256, 1024], P('dp')
- output 3: float32 [16, 256, 1024], P('dp')
- output 4: float32 [16, 256, 1024], P('dp')
- output 5: float32 [5, 1024, 3, 16, 64], P('dp', None, None, 'tp')
- output 6: float32 [5, 16, 64, 1024], P('dp', 'tp')
- output 7: float32 [5, 1024, 4096], P('dp', None, 'tp')
- output 8: float32 [5, 4096, 1024], P('dp', 'tp')
All inputs are finite; a program needn't handle non-finite values.
Results may differ from the reference program's by a relative error of at most 0.0127618.
Values are sent between devices in bfloat16 or wider.
A program may use at most 1 GiB of HBM per device.

```python
import jax
import jax.numpy as jnp
from jax import lax

SEQS = 16
SEQ = 256
HIDDEN = 1024
HEADS = 16
FF = 4096
PAIRS = 2

LAYERS = 2 * PAIRS + 1
HEAD = HIDDEN // HEADS
EPS = 1e-6


def setup_inputs(seed: int = 0, part: int = 0) -> dict:
    base_keys = jax.random.split(jax.random.key(seed), 2)
    act_keys = jax.random.split(jax.random.fold_in(base_keys[0], part), 6)
    w_keys = jax.random.split(base_keys[1], 4)
    state_shape = (SEQS, SEQ, HIDDEN)
    saved_shape = (PAIRS, SEQS, SEQ, HIDDEN)
    qk_gain = jnp.array([2.0 ** 0.5, 2.0 ** 0.5, 1.0], jnp.float32).reshape(1, 1, 3, 1, 1)
    wo_gain = 0.3 * (SEQ / 55.0) ** 0.5
    w_qkv = jax.random.normal(w_keys[0], (LAYERS, HIDDEN, 3, HEADS, HEAD), jnp.float32) * (HIDDEN ** -0.5) * qk_gain
    w_o = jax.random.normal(w_keys[1], (LAYERS, HEADS, HEAD, HIDDEN), jnp.float32) * (HIDDEN ** -0.5 * wo_gain)
    w_in = jax.random.normal(w_keys[2], (LAYERS, HIDDEN, FF), jnp.float32) * (HIDDEN ** -0.5)
    w_out = jax.random.normal(w_keys[3], (LAYERS, FF, HIDDEN), jnp.float32) * (0.45 * FF ** -0.5)
    return {
        "y_one": jax.random.normal(act_keys[0], state_shape, jnp.float32),
        "y_two": jax.random.normal(act_keys[1], state_shape, jnp.float32),
        "dy_one": jax.random.normal(act_keys[2], state_shape, jnp.float32),
        "dy_two": jax.random.normal(act_keys[3], state_shape, jnp.float32),
        "saved_one": jax.random.normal(act_keys[4], saved_shape, jnp.float32),
        "saved_two": jax.random.normal(act_keys[5], saved_shape, jnp.float32),
        "w_qkv": w_qkv.astype(jnp.bfloat16),
        "w_o": w_o.astype(jnp.bfloat16),
        "w_in": w_in.astype(jnp.bfloat16),
        "w_out": w_out.astype(jnp.bfloat16),
    }


def rms_norm(state):
    return state * lax.rsqrt(jnp.mean(state * state, axis=-1, keepdims=True) + EPS)


def to_bf(values):
    return values.astype(jnp.bfloat16).astype(jnp.float32)


def attend_one(qkv_one):
    q_one, k_one, v_one = qkv_one
    scores = jnp.einsum("qne,kne->nqk", q_one, k_one) * HEAD ** -0.5
    attn_probs = jax.nn.softmax(scores, axis=-1)
    return jnp.einsum("nqk,kne->qne", to_bf(attn_probs), v_one)


def branch_f(state, w_qkv, w_o):
    normed = to_bf(rms_norm(state))
    qkv_all = to_bf(jnp.einsum("bsh,hkne->kbsne", normed, w_qkv))
    heads_out = lax.map(jax.checkpoint(attend_one), (qkv_all[0], qkv_all[1], qkv_all[2]))
    return jnp.einsum("bsne,neh->bsh", to_bf(heads_out), w_o)


def branch_g(state, w_in, w_out):
    normed = to_bf(rms_norm(state))
    hidden = jnp.einsum("bsh,hf->bsf", normed, w_in)
    return jnp.einsum("bsf,fh->bsh", to_bf(jax.nn.gelu(hidden, approximate=True)), w_out)


def reversible_back(block_w, y_one, y_two, d_one, d_two):
    w_qkv, w_o, w_in, w_out = block_w
    g_val, g_pull = jax.vjp(branch_g, y_one, w_in, w_out)
    x_two = y_two - g_val
    g_dx, g_win, g_wout = g_pull(d_two)
    d_one = d_one + g_dx
    f_val, f_pull = jax.vjp(branch_f, x_two, w_qkv, w_o)
    x_one = y_one - f_val
    f_dx, f_wqkv, f_wo = f_pull(d_one)
    return x_one, x_two, d_one, d_two + f_dx, (f_wqkv, f_wo, g_win, g_wout)


def plain_back(block_w, x_one, x_two, d_one, d_two):
    w_qkv, w_o, w_in, w_out = block_w
    f_pull = jax.vjp(branch_f, x_two, w_qkv, w_o)[1]
    f_dx, f_wqkv, f_wo = f_pull(d_one)
    g_pull = jax.vjp(branch_g, x_one, w_in, w_out)[1]
    g_dx, g_win, g_wout = g_pull(d_two)
    return d_one + g_dx, d_two + f_dx, (f_wqkv, f_wo, g_win, g_wout)


def reference(y_one, y_two, dy_one, dy_two, saved_one, saved_two, w_qkv, w_o, w_in, w_out):
    weights = tuple(weight.astype(jnp.float32) for weight in (w_qkv, w_o, w_in, w_out))
    top_w = tuple(weight[LAYERS - 1] for weight in weights)
    x_one, x_two, d_one, d_two, top_grads = reversible_back(top_w, y_one, y_two, dy_one, dy_two)
    paired = tuple(weight[: 2 * PAIRS].reshape((PAIRS, 2) + weight.shape[1:]) for weight in weights)
    rev_w = tuple(weight[:, 0] for weight in paired)
    plain_w = tuple(weight[:, 1] for weight in paired)

    def pair_step(carry_in, scan_in):
        rev_block_w, plain_block_w, s_one, s_two = scan_in
        d_mid_one, d_mid_two, plain_grads = plain_back(plain_block_w, s_one, s_two, carry_in[2], carry_in[3])
        carry_out = reversible_back(rev_block_w, s_one, s_two, d_mid_one, d_mid_two)
        return carry_out[:4], (carry_out[4], plain_grads)

    final_state, scan_grads = lax.scan(pair_step, (x_one, x_two, d_one, d_two), (rev_w, plain_w, saved_one, saved_two), reverse=True)
    grad_out = tuple(
        jnp.concatenate([jnp.stack([rev_g, plain_g], axis=1).reshape((2 * PAIRS,) + rev_g.shape[1:]), top_g[None]], axis=0)
        for rev_g, plain_g, top_g in zip(scan_grads[0], scan_grads[1], top_grads)
    )
    return (final_state[0], final_state[1], final_state[2], final_state[3], grad_out[0], grad_out[1], grad_out[2], grad_out[3])
```

```python
import functools

import jax
import jax.numpy as jnp
from jax import lax
from jax.experimental import pallas as pl
from jax.experimental.pallas import tpu as pltpu
from jax.sharding import PartitionSpec as P

EPS = 1e-6
BF = jnp.bfloat16
F32 = jnp.float32
N = 8
VMEM = 60 * 1024 * 1024


def dot(a, b):
    return lax.dot_general(a, b, (((1,), (0,)), ((), ())), preferred_element_type=F32)


def dot_t(a, b):
    return lax.dot_general(a, b, (((1,), (1,)), ((), ())), preferred_element_type=F32)


def t_dot(a, b):
    return lax.dot_general(a, b, (((0,), (0,)), ((), ())), preferred_element_type=F32)


def rms_inv(x):
    return lax.rsqrt(jnp.mean(x * x, axis=-1, keepdims=True) + EPS)


def rms_pull(x, cot):
    r = rms_inv(x)
    return r * cot - x * (r * r * r * jnp.mean(x * cot, axis=-1, keepdims=True))


C0 = 0.7978845608028654
C1 = 0.044715


def gelu_parts(h):
    h2 = h * h
    t = jnp.tanh(h * (C0 + (C0 * C1) * h2))
    half = 0.5 * (1.0 + t)
    grad = half + (0.5 * h) * (1.0 - t * t) * (C0 + (3.0 * C0 * C1) * h2)
    return h * half, grad


def attend(qkv, d_heads, seq):
    rows, w3 = qkv.shape
    width = w3 // 3
    head = width // 2
    scale = head ** -0.5
    low = lax.broadcasted_iota(jnp.int32, (seq, width), 1) < head
    outs, grads = [], []
    for s in range(rows // seq):
        block = qkv[s * seq : (s + 1) * seq]
        qf = block[:, :width]
        q = qf.astype(BF)
        k = block[:, width : 2 * width].astype(BF)
        v = block[:, 2 * width :].astype(BF)
        if d_heads is not None:
            dof = d_heads[s * seq : (s + 1) * seq]
            do = dof.astype(BF)
        o_h, dq_h, dk_h, dv_h = [], [], [], []
        for h in range(2):
            mask = low if h == 0 else jnp.logical_not(low)
            q_m = jnp.where(mask, qf, 0.0).astype(BF)
            scores = dot_t(q_m, k) * scale
            e = jnp.exp(scores - jnp.max(scores, axis=-1, keepdims=True))
            probs = e * (1.0 / jnp.sum(e, axis=-1, keepdims=True))
            probs_b = probs.astype(BF)
            o_h.append(dot(probs_b, v))
            if d_heads is not None:
                do_m = jnp.where(mask, dof, 0.0).astype(BF)
                d_probs = dot_t(do_m, v)
                delta = jnp.sum(d_probs * probs, axis=-1, keepdims=True)
                ds = (probs * (d_probs - delta) * scale).astype(BF)
                dv_h.append(t_dot(probs_b, do))
                dq_h.append(dot(ds, k))
                dk_h.append(t_dot(ds, q))
        pick = lambda pair: jnp.where(low, pair[0], pair[1]).astype(BF)
        outs.append(pick(o_h))
        if d_heads is not None:
            grads.append(jnp.concatenate([pick(dq_h), pick(dk_h), pick(dv_h)], axis=1))
    o = jnp.concatenate(outs, axis=0)
    return o, (jnp.concatenate(grads, axis=0) if grads else None)


def call(body, grid, in_specs, out_specs, out_shape, scratch, sp, args, flops, nbytes, aliases=None):
    n_sp = 1
    return pl.pallas_call(
        body,
        grid_spec=pltpu.PrefetchScalarGridSpec(
            num_scalar_prefetch=n_sp, grid=grid, in_specs=in_specs, out_specs=out_specs, scratch_shapes=scratch
        ),
        out_shape=out_shape,
        input_output_aliases=aliases or {},
        compiler_params=pltpu.CompilerParams(
            dimension_semantics=("arbitrary",) * len(grid), vmem_limit_bytes=VMEM
        ),
        cost_estimate=pl.CostEstimate(flops=int(flops), bytes_accessed=int(nbytes), transcendentals=0),
    )(sp, *args)


def g_chain(sp, x, x_idx, d2, d2_idx, d1, d1_idx, weights, n_blk):
    rows, hid = d1.shape[1:]
    wr = weights.shape[1] // n_blk
    ff = wr // 2

    def body(sp_ref, x_ref, d2_ref, d1_ref, w_ref, out_ref, outb_ref, g_s, acc_s):
        step = pl.program_id(0)

        @pl.when(step == 0)
        def _():
            x_v = x_ref[0]
            g_s[...] = (x_v * rms_inv(x_v)).astype(BF)
            acc_s[...] = jnp.zeros_like(acc_s)

        w_in = w_ref[0, :ff]
        _, grad = gelu_parts(dot_t(g_s[...], w_in))
        d_act = dot_t(d2_ref[0].astype(BF), w_ref[0, ff:])
        acc_s[...] += dot((d_act * grad).astype(BF), w_in)

        @pl.when(step == N * n_blk - 1)
        def _():
            new = d1_ref[0] + rms_pull(x_ref[0], acc_s[...])
            out_ref[0] = new
            outb_ref[0] = new.astype(BF)

    tile = (1, rows, hid)
    return call(
        body,
        (N * n_blk,),
        [
            pl.BlockSpec(tile, lambda s, sp: (x_idx(sp), 0, 0)),
            pl.BlockSpec(tile, lambda s, sp: (d2_idx(sp, s // N), 0, 0)),
            pl.BlockSpec(tile, lambda s, sp: (d1_idx(sp), 0, 0)),
            pl.BlockSpec((1, wr, hid), lambda s, sp: (s % N, s // N, 0)),
        ],
        [pl.BlockSpec(tile, lambda s, sp: (0, 0, 0))] * 2,
        [jax.ShapeDtypeStruct(tile, F32), jax.ShapeDtypeStruct(tile, BF)],
        [pltpu.VMEM((rows, hid), BF), pltpu.VMEM((rows, hid), F32)],
        sp,
        (x, d2, d1, weights),
        6 * rows * hid * ff * N * n_blk,
        weights.size * 2 + 4 * rows * hid * 4,
    )


def f_chain(sp, xs, x_idxs, d1b, d2, d2_idx, weights, seq):
    n_blk = len(xs)
    rows, hid = d2.shape[1:]
    wr = weights.shape[1] // n_blk
    w3 = wr * 3 // 4

    def body(sp_ref, *refs):
        x_refs, (d1_ref, d2_ref, w_ref, out_ref, outb_ref, f_s, acc_s) = refs[:n_blk], refs[n_blk:]
        step = pl.program_id(0)

        @pl.when(step == 0)
        def _():
            out_ref[0] = d2_ref[0]

        for i in range(n_blk):

            @pl.when(step == N * i)
            def _():
                x_v = x_refs[i][0]
                f_s[...] = (x_v * rms_inv(x_v)).astype(BF)
                acc_s[...] = jnp.zeros_like(acc_s)

        w_q = w_ref[0, :w3]
        qkv = dot_t(f_s[...], w_q)
        d_heads = dot_t(d1_ref[0], w_ref[0, w3:])
        _, d_qkv = attend(qkv, d_heads, seq)
        acc_s[...] += dot(d_qkv, w_q)

        for i in range(n_blk):

            @pl.when(step == N * i + N - 1)
            def _():
                new = out_ref[0] + rms_pull(x_refs[i][0], acc_s[...])
                out_ref[0] = new
                outb_ref[0] = new.astype(BF)

    tile = (1, rows, hid)
    x_spec = lambda idx: pl.BlockSpec(tile, lambda s, sp: (idx(sp), 0, 0))
    return call(
        body,
        (N * n_blk,),
        [x_spec(idx) for idx in x_idxs]
        + [
            pl.BlockSpec(tile, lambda s, sp: (0, 0, 0)),
            pl.BlockSpec(tile, lambda s, sp: (d2_idx(sp), 0, 0)),
            pl.BlockSpec((1, wr, hid), lambda s, sp: (s % N, s // N, 0)),
        ],
        [pl.BlockSpec(tile, lambda s, sp: (0, 0, 0)), pl.BlockSpec(tile, lambda s, sp: (s // N, 0, 0))],
        [jax.ShapeDtypeStruct(tile, F32), jax.ShapeDtypeStruct((n_blk, rows, hid), BF)],
        [pltpu.VMEM((rows, hid), BF), pltpu.VMEM((rows, hid), F32)],
        sp,
        (*xs, d1b, d2, weights),
        24e9 * n_blk,
        weights.size * 2 + 6 * rows * hid * 4,
    )


def g_forward(sp, x_one, y_two, weights, blk, n_blk):
    half = N // 2
    per = 2
    rows, hid = x_one.shape[2:]
    wr = weights.shape[1] // n_blk
    ff = wr // 2
    m = per * rows

    def body(sp_ref, x_ref, y_ref, w_ref, out_ref, outb_ref, g_s, acc_s):
        j = pl.program_id(1)

        @pl.when(j == 0)
        def _():
            x_v = x_ref[...].reshape(m, hid)
            g_s[...] = (x_v * rms_inv(x_v)).astype(BF)
            acc_s[...] = jnp.zeros_like(acc_s)

        act, _ = gelu_parts(dot_t(g_s[...], w_ref[0, :ff]))
        acc_s[...] += dot(act.astype(BF), w_ref[0, ff:])

        @pl.when(j == N - 1)
        def _():
            x_two = y_ref[...].reshape(m, hid) - acc_s[...]
            out_ref[...] = x_two.reshape(per, rows, hid)
            outb_ref[...] = (x_two * rms_inv(x_two)).astype(BF).reshape(per, rows, hid)

    tile = (per, 1, rows, hid)
    return call(
        body,
        (half // per, N),
        [
            pl.BlockSpec(tile, lambda i, j, sp: (i, sp[1], 0, 0)),
            pl.BlockSpec(tile, lambda i, j, sp: (i, sp[1], 0, 0)),
            pl.BlockSpec((1, wr, hid), lambda i, j, sp: (j, blk, 0)),
        ],
        [pl.BlockSpec((per, rows, hid), lambda i, j, sp: (i, 0, 0))] * 2,
        [jax.ShapeDtypeStruct((half, rows, hid), F32), jax.ShapeDtypeStruct((half, rows, hid), BF)],
        [pltpu.VMEM((m, hid), BF), pltpu.VMEM((m, hid), F32)],
        sp,
        (x_one, y_two, weights),
        4 * half * rows * hid * ff * N,
        half * rows * hid * 14 + 2 * N * wr * hid * half // per,
    )


def f_forward(sp, f_in, y_one, weights, seq):
    half, rows, hid = f_in.shape
    wr = weights.shape[1]
    w3 = wr * 3 // 4

    def body(sp_ref, f_ref, y_ref, w_ref, out_ref, acc_s):
        j = pl.program_id(1)

        @pl.when(j == 0)
        def _():
            acc_s[...] = jnp.zeros_like(acc_s)

        qkv = dot_t(f_ref[0], w_ref[0, :w3])
        o, _ = attend(qkv, None, seq)
        acc_s[...] += dot(o, w_ref[0, w3:])

        @pl.when(j == N - 1)
        def _():
            out_ref[0] = y_ref[0, 0] - acc_s[...]

    tile = (1, rows, hid)
    return call(
        body,
        (half, N),
        [
            pl.BlockSpec(tile, lambda i, j, sp: (i, 0, 0)),
            pl.BlockSpec((1, 1, rows, hid), lambda i, j, sp: (i, sp[1], 0, 0)),
            pl.BlockSpec((1, wr, hid), lambda i, j, sp: (j, 0, 0)),
        ],
        pl.BlockSpec(tile, lambda i, j, sp: (i, 0, 0)),
        jax.ShapeDtypeStruct((half, rows, hid), F32),
        [pltpu.VMEM((rows, hid), F32)],
        sp,
        (f_in, y_one, weights),
        50e9,
        half * rows * hid * 10 + 2 * N * wr * hid * half,
    )


def g_grads(sp, x_one, d2, d2_idx, w_in, w_out, top_blk, n_blk, prev):
    rows, hid = x_one.shape[1:]
    n_layers, _, ff = w_in.shape

    def body(sp_ref, x_ref, d2_ref, wi_ref, wo_ref, *rest):
        dwi_ref, dwo_ref = rest[-2:]
        t = pl.program_id(1)
        x_v = x_ref[0]
        g = (x_v * rms_inv(x_v)).astype(BF)
        d2_v = d2_ref[...].reshape(rows, hid).astype(BF)
        act, grad = gelu_parts(dot(g, wi_ref[0]))
        d_hidden = (dot_t(d2_v, wo_ref[0]) * grad).astype(BF)
        dwi = t_dot(g, d_hidden)
        dwo = t_dot(act.astype(BF), d2_v)

        @pl.when(t == 0)
        def _():
            dwi_ref[0] = dwi
            dwo_ref[0] = dwo

        @pl.when(t > 0)
        def _():
            dwi_ref[0] += dwi
            dwo_ref[0] += dwo

    any_spec = pl.BlockSpec(memory_space=pl.ANY)
    d2_tile = (1,) * (d2.ndim - 2) + (rows, hid)
    return call(
        body,
        (n_blk, N),
        [
            pl.BlockSpec((1, rows, hid), lambda b, t, sp: (t, 0, 0)),
            pl.BlockSpec(d2_tile, lambda b, t, sp: d2_idx(b, t)),
            pl.BlockSpec((1, hid, ff), lambda b, t, sp: (top_blk - b, 0, 0)),
            pl.BlockSpec((1, ff, hid), lambda b, t, sp: (top_blk - b, 0, 0)),
        ]
        + [any_spec] * len(prev),
        [
            pl.BlockSpec((1, hid, ff), lambda b, t, sp: (top_blk - b, 0, 0)),
            pl.BlockSpec((1, ff, hid), lambda b, t, sp: (top_blk - b, 0, 0)),
        ],
        [jax.ShapeDtypeStruct((n_layers, hid, ff), F32), jax.ShapeDtypeStruct((n_layers, ff, hid), F32)],
        [],
        sp,
        (x_one, d2, w_in, w_out, *prev),
        8 * N * rows * hid * ff * n_blk,
        n_blk * N * rows * hid * 6,
        {5 + i: i for i in range(len(prev))},
    )


def f_grads(sp, f_ins, d1, w_qkv, w_o, blk, prev, seq):
    rows, hid = d1.shape[1:]
    n_layers, w3, _ = w_qkv.shape
    w1 = w_o.shape[1]
    half = N // 2
    two = len(f_ins) == 2

    def body(sp_ref, *refs):
        d1_ref, wq_ref, wo_ref = refs[len(f_ins) : len(f_ins) + 3]
        dwq_ref, dwo_ref, f_s = refs[-3:]
        t = pl.program_id(0)
        if two:

            @pl.when(t < half)
            def _():
                f_s[...] = refs[0][0]

            @pl.when(t >= half)
            def _():
                f_s[...] = refs[1][0]
        else:
            x_v = refs[0][0]
            f_s[...] = (x_v * rms_inv(x_v)).astype(BF)
        d1_v = d1_ref[0].astype(BF)
        qkv = dot_t(f_s[...], wq_ref[0])
        d_heads = dot_t(d1_v, wo_ref[0])
        o, d_qkv = attend(qkv, d_heads, seq)
        dwq = t_dot(d_qkv, f_s[...])
        dwo = t_dot(o, d1_v)

        @pl.when(t == 0)
        def _():
            dwq_ref[0] = dwq
            dwo_ref[0] = dwo

        @pl.when(t > 0)
        def _():
            dwq_ref[0] += dwq
            dwo_ref[0] += dwo

    any_spec = pl.BlockSpec(memory_space=pl.ANY)
    tile = (1, rows, hid)
    if two:
        f_specs = [
            pl.BlockSpec(tile, lambda t, sp: (jnp.minimum(t, half - 1), 0, 0)),
            pl.BlockSpec(tile, lambda t, sp: (jnp.maximum(t - half, 0), 0, 0)),
        ]
        d1_spec = pl.BlockSpec(tile, lambda t, sp: (2 * (t % half) + (t // half + sp[1]) % 2, 0, 0))
    else:
        f_specs = [pl.BlockSpec(tile, lambda t, sp: (t, 0, 0))]
        d1_spec = pl.BlockSpec(tile, lambda t, sp: (t, 0, 0))
    w_spec = lambda w: pl.BlockSpec((1, w, hid), lambda t, sp: (blk, 0, 0))
    n_in = len(f_ins) + 3
    return call(
        body,
        (N,),
        f_specs + [d1_spec, w_spec(w3), w_spec(w1)] + [any_spec] * len(prev),
        [w_spec(w3), w_spec(w1)],
        [jax.ShapeDtypeStruct((n_layers, w3, hid), F32), jax.ShapeDtypeStruct((n_layers, w1, hid), F32)],
        [pltpu.VMEM((rows, hid), BF)],
        sp,
        (*f_ins, d1, w_qkv, w_o, *prev),
        28e9,
        N * rows * hid * 6,
        {1 + n_in + i: i for i in range(len(prev))},
    )


def solution(mesh):
    act_spec = P("dp", None, None)
    saved_spec = P(None, "dp", None, None)
    weight_specs = (P(None, None, None, "tp", None), P(None, "tp", None, None), P(None, None, "tp"), P(None, "tp", None))
    grad_specs = (P("dp", None, None, "tp", None), P("dp", "tp", None, None), P("dp", None, "tp"), P("dp", "tp", None))
    core_pairs = [(i, i ^ 1) for i in range(N)]

    def gather(x):
        return lax.all_gather(x, "tp", axis=0, tiled=False)

    def per_device(y_one, y_two, dy_one, dy_two, saved_one, saved_two, w_qkv, w_o, w_in, w_out):
        seqs, seq, hid = y_one.shape
        n_layers = w_qkv.shape[0]
        n_pairs = saved_one.shape[0]
        rows = seqs * seq // N
        me = lax.axis_index("tp")
        core = me % 2
        sp = jnp.stack([me, core, me // 2]).astype(jnp.int32)

        tiles = lambda x: x.reshape(N, rows, hid)
        pairs = lambda x: x.reshape(N // 2, 2, rows, hid)
        own = lambda sp: sp[0]
        in_half = lambda sp: sp[2]
        first = lambda sp: 0

        wq_t = jnp.transpose(w_qkv, (0, 2, 3, 4, 1)).reshape(n_layers, -1, hid)
        wo_t = w_o.reshape(n_layers, -1, hid)
        g_bundle = lambda b: jnp.concatenate([w_in[b].T, w_out[b]], axis=0)
        f_bundle = lambda b: jnp.concatenate([wq_t[b], wo_t[b]], axis=0)

        def swap(x):
            return lax.ppermute(x, "tp", core_pairs)

        def whole(half_own):
            other = swap(half_own)
            even = jnp.where(core == 0, half_own, other)
            odd = jnp.where(core == 0, other, half_own)
            return jnp.stack([even, odd], axis=1).reshape(seqs, seq, hid)

        top = n_layers - 1
        wg = gather(g_bundle(top))
        wf = gather(jnp.concatenate([f_bundle(top), f_bundle(top - 1)], axis=0)) if n_pairs else gather(f_bundle(0))
        g_acc = g_grads(sp, tiles(y_one), tiles(dy_two), lambda b, t: (t, 0, 0), w_in, w_out, top, 1, ())
        x2h, f_h = g_forward(sp, pairs(y_one), pairs(y_two), wg, 0, 1)
        d1, d1b = g_chain(
            sp, tiles(y_one), own, tiles(dy_two), lambda sp, b: sp[0], tiles(dy_one), own, wg, 1
        )
        d2, d2_idx = tiles(dy_two), own
        f_acc = ()
        y1 = y_one
        for pair in reversed(range(n_pairs)):
            rev = 2 * pair + 2
            s_one, s_two = saved_one[pair], saved_two[pair]
            d1_all = gather(d1b[0])
            wg = gather(jnp.concatenate([g_bundle(rev - 1), g_bundle(rev - 2)], axis=0))
            d2, d2b = f_chain(sp, (x2h, tiles(s_two)), (in_half, own), d1b, d2, d2_idx, wf, seq)
            d2_idx = first
            nxt = rev - 2
            wf = gather(f_bundle(0)) if pair == 0 else gather(jnp.concatenate([f_bundle(nxt), f_bundle(nxt - 1)], axis=0))
            d2_all = gather(d2b)
            f_acc = f_grads(sp, (f_h, swap(f_h)), d1_all, wq_t, wo_t, rev, f_acc, seq)
            f_acc = f_grads(sp, (tiles(s_two),), d1_all, wq_t, wo_t, rev - 1, f_acc, seq)
            x2h, f_h = g_forward(sp, pairs(s_one), pairs(s_two), wg, 1, 2)
            d1, d1b = g_chain(sp, tiles(s_one), own, d2b, lambda sp, b: b, d1, first, wg, 2)
            g_acc = g_grads(
                sp, tiles(s_one), d2_all, lambda b, t: (t, b, 0, 0), w_in, w_out, rev - 1, 2, g_acc
            )
            y1 = s_one
        d1_all = gather(d1[0])
        x_two = whole(x2h)
        x_one = whole(f_forward(sp, f_h, pairs(y1), wf, seq))
        d2, _ = f_chain(sp, (x2h,), (in_half,), d1b, d2, d2_idx, wf, seq)
        d2_all = gather(d2[0])
        f_acc = f_grads(sp, (f_h, swap(f_h)), d1_all, wq_t, wo_t, 0, f_acc, seq)

        head = w_qkv.shape[-1]
        dwq = jnp.transpose(f_acc[0].reshape(n_layers, 3, -1, head, hid), (0, 4, 1, 2, 3))
        dwo = f_acc[1].reshape(w_o.shape)
        shape = (seqs, seq, hid)
        return (x_one, x_two, d1_all.reshape(shape), d2_all.reshape(shape), dwq, dwo) + tuple(g_acc)

    return jax.shard_map(
        per_device,
        mesh=mesh,
        in_specs=(act_spec,) * 4 + (saved_spec,) * 2 + weight_specs,
        out_specs=(act_spec,) * 4 + grad_specs,
        check_vma=False,
    )
```
